32 devices in a mesh: row: 4 (over x, core), col: 8 (over z, y).
Axes of the slice: x: 2, y: 2, z: 4, core: 2. Of those that a mesh axis runs over, the one named last changes fastest.
Arguments:
- rhs: float32 [4, 8, 8, 4, 128], P('row', 'col'), may hold values from -6 to 6
- diag0: float32 [4, 8, 8, 128], P('row', 'col'), may hold values from 2 to 4
- blocks0: float32 [4, 8, 8, 14, 128, 128], P('row', 'col'), may hold values from -0.1875 to 0.1875
- cols0: int32 [4, 8, 8, 14], P('row', 'col'), may hold values from 0 to 23
- sends0: int32 [4, 8, 4, 4], P('row', 'col'), may hold values from 0 to 7
- pro0: float32 [4, 8, 8, 128, 128], P('row', 'col'), may hold values from -0.5 to 0.5
- agg0: int32 [4, 8, 8], P('row', 'col'), may hold values from 0 to 1
- diag1: float32 [4, 8, 2, 128], P('row', 'col'), may hold values from 2 to 4
- blocks1: float32 [4, 8, 2, 14, 128, 128], P('row', 'col'), may hold values from -0.1875 to 0.1875
- cols1: int32 [4, 8, 2, 14], P('row', 'col'), may hold values from 0 to 9
- sends1: int32 [4, 8, 4, 2], P('row', 'col'), may hold values from 0 to 1
- pro1: float32 [4, 8, 2, 128, 128], P('row', 'col'), may hold values from -0.25 to 0.25
- agg1: int32 [4, 8, 2], P('row', 'col'), may hold values from 0 to 7
- cinv: float32 [1024, 1024], P(('row', 'col')), may hold values from -0.1875 to 0.1875
Outputs:
- solution: float32 [4, 8, 8, 4, 128], P('row', 'col')
The draws below stay inside these ranges and needn't reach their ends.
Inputs may be any that keep to these rules, and one draw needn't show every extreme that they name: `sends0`: indices of the sender's own fine blocks. `sends1`: indices of the sender's own level-one blocks. `cols0`: indices into the extended fine vector of 24 blocks. `cols1`: indices into the extended level-one vector of 10 blocks. `agg0`: a level-one block of the same partition. `agg1`: a coarsest block, on any partition.
All inputs are finite; a program needn't handle non-finite values.
Results may differ from the reference program's by a relative error of at most 0.0001.
Values sent between devices are 32-bit elements; how exact they have to be, the bound alone decides.
A program may use at most 64 MiB of HBM per device.

```python
import math
import jax
import jax.numpy as jnp
from jax import lax

BS = 128
NB = 8
NB1 = 2
K = 14
K1 = 14
G0 = 4
G1 = 2
NRHS = 4
NU = 2
NCB = 8
NCU = 1024
N_ROW = 4
N_COL = 8


def touch_ends(result, key, least, top_value):
    place = [jax.random.randint(jax.random.fold_in(key, axis), (), 0, length) for axis, length in enumerate(result.shape)]
    longest = result.shape.index(max(result.shape))
    next_to = place[:longest] + [(place[longest] + 1) % result.shape[longest]] + place[longest + 1:]
    return result.at[tuple(place)].set(least).at[tuple(next_to)].set(top_value)


def steps_of(stream_key, shape, shards, least, largest):
    gain = 1.0
    for dim, blocks in shards:
        steps = jax.random.uniform(jax.random.fold_in(jax.random.fold_in(stream_key, 6), dim), (blocks,), jnp.float32, least / len(shards), largest / len(shards))
        gain = gain * jnp.repeat(jnp.exp(steps), shape[dim] // blocks).reshape((-1,) + (1,) * (len(shape) - 1 - dim))
    return gain


def bell_draw(key, shape, spread, most, cuts=(), dtype=jnp.bfloat16):
    drawn = jax.random.normal(key, shape, jnp.float32) * spread
    if len(cuts) > 0:
        drawn = steps_of(key, shape, cuts, -0.22, 0.18) * drawn
    return jnp.clip(drawn, min=-most, max=most).astype(dtype)


def setup_inputs(seed: int = 0) -> dict:
    splits = jax.random.split(jax.random.key(seed), 15)
    rhs = bell_draw(splits[0], (N_ROW, N_COL, NB, NRHS, BS), 1.0, 6.0, ((0, 4), (1, 8)), jnp.float32)
    diag0 = jnp.clip(jnp.exp(math.log(4.0) - 0.6931472 * jax.random.uniform(splits[1], (N_ROW, N_COL, NB, BS), jnp.float32) ** steps_of(splits[1], (N_ROW, N_COL, NB, BS), ((0, 4), (1, 8)), -0.2, 0.2)), 2.0, 4.0)
    blocks0 = bell_draw(splits[2], (N_ROW, N_COL, NB, K, BS, BS), (K * BS // 2) ** -0.5, 0.1875, ((0, 4), (1, 8)), jnp.float32)
    cols0 = touch_ends(jax.random.randint(splits[3], (N_ROW, N_COL, NB, K), 0, NB + 4 * G0), jax.random.fold_in(splits[3], 1), 0, (NB + 4 * G0) - 1).astype(jnp.int32)
    sends0 = touch_ends(jax.random.randint(splits[4], (N_ROW, N_COL, 4, G0), 0, NB), jax.random.fold_in(splits[4], 1), 0, NB - 1).astype(jnp.int32)
    pro0 = bell_draw(splits[5], (N_ROW, N_COL, NB, BS, BS), BS ** -0.5, 0.5, ((0, 4), (1, 8)), jnp.float32)
    agg0 = touch_ends(jax.random.randint(splits[6], (N_ROW, N_COL, NB), 0, NB1), jax.random.fold_in(splits[6], 1), 0, NB1 - 1).astype(jnp.int32)
    diag1 = jnp.clip(jnp.exp(math.log(4.0) - 0.6931472 * jax.random.uniform(splits[7], (N_ROW, N_COL, NB1, BS), jnp.float32) ** steps_of(splits[7], (N_ROW, N_COL, NB1, BS), ((0, 4), (1, 8)), -0.2, 0.2)), 2.0, 4.0)
    blocks1 = bell_draw(splits[8], (N_ROW, N_COL, NB1, K1, BS, BS), (K1 * BS // 2) ** -0.5, 0.1875, ((0, 4), (1, 8)), jnp.float32)
    cols1 = touch_ends(jax.random.randint(splits[9], (N_ROW, N_COL, NB1, K1), 0, NB1 + 4 * G1), jax.random.fold_in(splits[9], 1), 0, (NB1 + 4 * G1) - 1).astype(jnp.int32)
    sends1 = touch_ends(jax.random.randint(splits[10], (N_ROW, N_COL, 4, G1), 0, NB1), jax.random.fold_in(splits[10], 1), 0, NB1 - 1).astype(jnp.int32)
    pro1 = bell_draw(splits[11], (N_ROW, N_COL, NB1, BS, BS), (4 * BS) ** -0.5, 0.25, ((0, 4), (1, 8)), jnp.float32)
    agg1 = touch_ends(jax.random.randint(splits[12], (N_ROW, N_COL, NB1), 0, NCB), jax.random.fold_in(splits[12], 1), 0, NCB - 1).astype(jnp.int32)
    cinv = bell_draw(splits[13], (NCU, NCU), NCU ** -0.5, 0.1875, ((0, 32),), jnp.float32)
    return dict(rhs=rhs, diag0=diag0, blocks0=blocks0, cols0=cols0, sends0=sends0, pro0=pro0, agg0=agg0, diag1=diag1, blocks1=blocks1, cols1=cols1, sends1=sends1, pro1=pro1, agg1=agg1, cinv=cinv)


HIGH = lax.Precision.HIGHEST
OMEGA = 0.3


def gather_ghosts(vector, sends):
    packed = jax.vmap(jax.vmap(lambda blocks, picks: blocks[picks]))(vector, sends)
    zero_row = jnp.zeros_like(packed[:1, :, 0])
    zero_col = jnp.zeros_like(packed[:, :1, 0])
    above = jnp.concatenate([zero_row, packed[:-1, :, 0]], axis=0)
    below = jnp.concatenate([packed[1:, :, 1], zero_row], axis=0)
    left = jnp.concatenate([zero_col, packed[:, :-1, 2]], axis=1)
    right = jnp.concatenate([packed[:, 1:, 3], zero_col], axis=1)
    return jnp.concatenate([vector, above, below, left, right], axis=2)


def apply_op(vector, diag, blocks, cols, sends):
    extended = gather_ghosts(vector, sends)
    nearby = jax.vmap(jax.vmap(lambda source, picks: source[picks]))(extended, cols)
    coupled = jnp.einsum('xybkij,xybkrj->xybri', blocks, nearby, precision=HIGH)
    return diag[..., None, :] * vector + coupled


def smooth(vector, right_side, diag, blocks, cols, sends, count):
    for sweep in range(count):
        vector = vector + OMEGA * (right_side - apply_op(vector, diag, blocks, cols, sends)) / diag[..., None, :]
    return vector


def reference(rhs, diag0, blocks0, cols0, sends0, pro0, agg0, diag1, blocks1, cols1, sends1, pro1, agg1, cinv):
    fine_x = OMEGA * rhs / diag0[..., None, :]
    fine_x = smooth(fine_x, rhs, diag0, blocks0, cols0, sends0, NU - 1)
    fine_res = rhs - apply_op(fine_x, diag0, blocks0, cols0, sends0)
    onehot0 = (agg0[..., None] == jnp.arange(NB1)).astype(jnp.float32)
    restricted = jnp.einsum('xybij,xybri->xybrj', pro0, fine_res, precision=HIGH)
    level_rhs = jnp.einsum('xybc,xybrj->xycrj', onehot0, restricted, precision=HIGH)
    level_x = OMEGA * level_rhs / diag1[..., None, :]
    level_x = smooth(level_x, level_rhs, diag1, blocks1, cols1, sends1, NU - 1)
    level_res = level_rhs - apply_op(level_x, diag1, blocks1, cols1, sends1)
    onehot1 = (agg1[..., None] == jnp.arange(NCB)).astype(jnp.float32)
    contrib = jnp.einsum('xybij,xybri->xybrj', pro1, level_res, precision=HIGH)
    coarse_rhs = jnp.einsum('xybc,xybrj->rcj', onehot1, contrib, precision=HIGH).reshape(NRHS, NCU)
    coarse_x = jnp.einsum('ij,rj->ri', cinv, coarse_rhs, precision=HIGH)
    coarse_blocks = coarse_x.reshape(NRHS, NCB, BS)
    picked = jnp.einsum('xybc,rcj->xybrj', onehot1, coarse_blocks, precision=HIGH)
    level_x = level_x + jnp.einsum('xybij,xybrj->xybri', pro1, picked, precision=HIGH)
    level_x = smooth(level_x, level_rhs, diag1, blocks1, cols1, sends1, NU)
    lifted = jnp.einsum('xybc,xycrj->xybrj', onehot0, level_x, precision=HIGH)
    fine_x = fine_x + jnp.einsum('xybij,xybrj->xybri', pro0, lifted, precision=HIGH)
    fine_x = smooth(fine_x, rhs, diag0, blocks0, cols0, sends0, NU)
    return fine_x
```

```python
import functools

import jax
import jax.numpy as jnp
from jax import lax
from jax.experimental import pallas as pl
from jax.experimental.pallas import tpu as pltpu
from jax.sharding import PartitionSpec as P

NU = 2
OMEGA = 0.3
F32 = jnp.float32
BF16 = jnp.bfloat16
MESH = pl.DeviceIdType.MESH
NT = (((1,), (1,)), ((), ()))
NN = (((1,), (0,)), ((), ()))


def two_terms(value):
    head = value.astype(BF16)
    tail = (value - head.astype(F32)).astype(BF16)
    return head, tail


def stacked(value):
    head = value.astype(BF16).astype(F32)
    rows = 2 * value.shape[0]
    pad = -rows % 16
    parts = [head, value - head]
    if pad:
        parts.append(jnp.zeros((pad, value.shape[1]), F32))
    return jnp.concatenate(parts, axis=0).astype(BF16)


def product(lhs, head, tail, dims, rows):
    both = lax.dot_general(lhs, head, dims, preferred_element_type=F32) + lax.dot_general(
        lhs, tail, dims, preferred_element_type=F32
    )
    return both[:rows] + both[rows : 2 * rows]


def kernel(
    n_row, n_col,
    cols0, sends0, agg0, cols1, sends1, agg1,
    rhs_h, diag0_h, blocks0_h, pro0_h, diag1_h, blocks1_h, pro1_h, cinv_h,
    out,
    rhs, diag0, blocks0, pro0, diag1, blocks1, pro1, cinv,
    in_sem,
    head0, tail0, head1, tail1, phead0, ptail0, phead1, ptail1, chead, ctail,
    dfull0, wfull0, dfull1, wfull1,
    ext0, ext1, x0, x1, b1,
    send0, recv0, send1, recv1,
    aggf, recva, mine, recvc, xs, recvx,
    s_send0, s_recv0, s_send1, s_recv1, s_bsend, s_brecv,
):
    nb, loads, bs = rhs.shape
    nb1 = diag1.shape[0]
    k0 = blocks0.shape[1]
    k1 = blocks1.shape[1]
    g0 = send0.shape[2]
    g1 = send1.shape[2]
    n = n_row * n_col
    owned = cinv.shape[0]
    ncb = cinv.shape[1] // bs
    reps = bs // owned
    row = lax.axis_index("row")
    col = lax.axis_index("col")
    me = row * n_col + col

    def peer(step):
        other = lax.rem(me + step, n)
        return (other // n_col, lax.rem(other, n_col))

    loading = []

    def load(source, target):
        copy = pltpu.make_async_copy(source, target, in_sem.at[len(loading)])
        loading.append(copy)
        copy.start()
        return copy

    l_rhs = load(rhs_h, rhs)
    l_diag0 = load(diag0_h, diag0)
    l_blocks0 = [load(blocks0_h.at[b], blocks0.at[b]) for b in range(nb)]
    l_pro0 = load(pro0_h, pro0)
    l_diag1 = load(diag1_h, diag1)
    l_blocks1 = load(blocks1_h, blocks1)
    l_pro1 = load(pro1_h, pro1)
    l_cinv = load(cinv_h, cinv)

    recv0[...] = jnp.zeros_like(recv0)
    recv1[...] = jnp.zeros_like(recv1)

    barrier = pltpu.get_barrier_semaphore()

    def greet(step, carry):
        pl.semaphore_signal(barrier, inc=1, device_id=peer(step), device_id_type=MESH)
        return carry

    lax.fori_loop(1, n, greet, 0)

    directions = (
        (row < n_row - 1, (row + 1, col), row > 0),
        (row > 0, (row - 1, col), row < n_row - 1),
        (col < n_col - 1, (row, col + 1), col > 0),
        (col > 0, (row, col - 1), col < n_col - 1),
    )

    def halo_copy(send, recv, s_send, s_recv, e, d, there):
        return pltpu.make_async_remote_copy(
            src_ref=send.at[e, d], dst_ref=recv.at[e, d],
            send_sem=s_send.at[e, d], recv_sem=s_recv.at[e, d],
            device_id=there, device_id_type=MESH,
        )

    def pack(x, send, sends, e):
        for d in range(4):
            for g in range(send.shape[2]):
                send[e, d, g] = x[sends[d, g]]

    def start(send, recv, s_send, s_recv, e):
        for d, (goes, there, _) in enumerate(directions):
            @pl.when(goes)
            def _():
                halo_copy(send, recv, s_send, s_recv, e, d, there).start()

    def finish(send, recv, s_send, s_recv, e):
        for d, (_, there, comes) in enumerate(directions):
            @pl.when(comes)
            def _():
                halo_copy(send, recv, s_send, s_recv, e, d, (row, col)).wait_recv()

    def drain(send, recv, s_send, s_recv, e):
        for d, (goes, there, _) in enumerate(directions):
            @pl.when(goes)
            def _():
                halo_copy(send, recv, s_send, s_recv, e, d, there).wait_send()

    level0 = (send0, recv0, s_send0, s_recv0)
    level1 = (send1, recv1, s_send1, s_recv1)

    def own_ext(x, ext, count):
        for b in range(count):
            ext[b] = stacked(x[b])

    def ghost_ext(recv, ext, count, e):
        ghosts = recv.shape[2]
        for d in range(4):
            for g in range(ghosts):
                ext[count + d * ghosts + g] = stacked(recv[e, d, g])

    def coupled(b, cols, ext, head, tail, k):
        lhs = jnp.concatenate([ext[cols[b, i]] for i in range(k)], axis=1)
        return product(lhs, head[b], tail[b], NT, loads)

    def split_blocks(b, blocks, head, tail, k):
        def one(i, carry):
            h, t = two_terms(blocks[b, i])
            at = pl.ds(pl.multiple_of(i * bs, bs), bs)
            head[b, :, at] = h
            tail[b, :, at] = t
            return carry

        lax.fori_loop(0, k, one, 0)

    l_rhs.wait()
    l_diag0.wait()
    for b in range(nb):
        d = jnp.broadcast_to(diag0[b : b + 1, :], (loads, bs))
        w = OMEGA / d
        dfull0[b] = d
        wfull0[b] = w
        x0[b] = w * rhs[b]
    pack(x0, send0, sends0, 0)
    for b in range(nb1):
        aggf[b * loads : (b + 1) * loads, :] = jnp.full((loads, bs), agg1[b].astype(F32))
    recva[me] = aggf[...]
    pl.semaphore_wait(barrier, n - 1)
    start(*level0, 0)

    def everywhere(src, dst, which):
        def one(step, carry):
            pltpu.make_async_remote_copy(
                src_ref=src, dst_ref=dst.at[me],
                send_sem=s_bsend.at[which], recv_sem=s_brecv.at[which],
                device_id=peer(step), device_id_type=MESH,
            ).start()
            return carry

        lax.fori_loop(1, n, one, 0)

    def all_bytes(dst, sem):
        part = dst.at[pl.ds(0, n - 1)]
        pltpu.make_async_copy(part, part, sem).wait()

    everywhere(aggf, recva, 0)
    own_ext(x0, ext0, nb)
    for b in range(nb):
        l_blocks0[b].wait()
        split_blocks(b, blocks0, head0, tail0, k0)

    def sweep0(e, into):
        finish(*level0, e)
        ghost_ext(recv0, ext0, nb, e)
        for b in range(nb):
            c = coupled(b, cols0, ext0, head0, tail0, k0)
            v = x0[b]
            into[b] = v + wfull0[b] * (rhs[b] - (dfull0[b] * v + c))

    def sweep1(e, right, into):
        finish(*level1, e)
        ghost_ext(recv1, ext1, nb1, e)
        for b in range(nb1):
            c = coupled(b, cols1, ext1, head1, tail1, k1)
            v = x1[b]
            into[b] = v + wfull1[b] * (right[b] - (dfull1[b] * v + c))

    e0 = 0
    for _ in range(NU - 1):
        sweep0(e0, x0)
        e0 += 1
        pack(x0, send0, sends0, e0)
        start(*level0, e0)
        own_ext(x0, ext0, nb)

    l_pro0.wait()
    for b in range(nb):
        h, t = two_terms(pro0[b])
        phead0[b] = h
        ptail0[b] = t
    l_blocks1.wait()
    for b in range(nb1):
        split_blocks(b, blocks1, head1, tail1, k1)
    l_diag1.wait()
    for b in range(nb1):
        d = jnp.broadcast_to(diag1[b : b + 1, :], (loads, bs))
        dfull1[b] = d
        wfull1[b] = OMEGA / d

    finish(*level0, e0)
    ghost_ext(recv0, ext0, nb, e0)
    sums = [jnp.zeros((loads, bs), F32) for _ in range(nb1)]
    for b in range(nb):
        c = coupled(b, cols0, ext0, head0, tail0, k0)
        r = rhs[b] - (dfull0[b] * x0[b] + c)
        q = product(stacked(r), phead0[b], ptail0[b], NN, loads)
        for a in range(nb1):
            sums[a] = sums[a] + jnp.where(agg0[b] == a, q, 0.0)
    e0 += 1

    for b in range(nb1):
        b1[b] = sums[b]
        x1[b] = wfull1[b] * sums[b]
    pack(x1, send1, sends1, 0)
    start(*level1, 0)
    own_ext(x1, ext1, nb1)
    l_pro1.wait()
    for b in range(nb1):
        h, t = two_terms(pro1[b])
        phead1[b] = h
        ptail1[b] = t
    l_cinv.wait()
    h, t = two_terms(cinv[...])
    chead[...] = h
    ctail[...] = t
    e1 = 0
    for _ in range(NU - 1):
        sweep1(e1, b1, x1)
        e1 += 1
        pack(x1, send1, sends1, e1)
        start(*level1, e1)
        own_ext(x1, ext1, nb1)
    finish(*level1, e1)
    ghost_ext(recv1, ext1, nb1, e1)
    for b in range(nb1):
        c = coupled(b, cols1, ext1, head1, tail1, k1)
        r = b1[b] - (dfull1[b] * x1[b] + c)
        q = product(stacked(r), phead1[b], ptail1[b], NN, loads)
        mine[b * loads : (b + 1) * loads, :] = q
    e1 += 1

    everywhere(mine, recvc, 1)
    recvc[me] = mine[...]
    all_bytes(recva, s_brecv.at[0])
    all_bytes(recvc, s_brecv.at[1])
    index = lax.broadcasted_iota(jnp.int32, (ncb, nb1 * loads, bs), 0).astype(F32)

    def collect(d, total):
        return total + jnp.where(recva[d][None] == index, recvc[d][None], 0.0)

    total = lax.fori_loop(
        0, n, collect, jnp.zeros((ncb, nb1 * loads, bs), F32), unroll=4
    )
    pieces = []
    for c in range(ncb):
        piece = total[c, :loads]
        for b in range(1, nb1):
            piece = piece + total[c, b * loads : (b + 1) * loads]
        pieces.append(stacked(piece))
    own = product(jnp.concatenate(pieces, axis=1), chead[...], ctail[...], NT, loads)
    wide = jnp.concatenate([own] * reps, axis=1)
    lane = lax.broadcasted_iota(jnp.int32, (loads, bs), 1)
    low = lax.rem(me, reps) * owned
    xs[...] = jnp.where((lane >= low) & (lane < low + owned), wide, 0.0)
    everywhere(xs, recvx, 2)
    recvx[me] = xs[...]
    all_bytes(recvx, s_brecv.at[2])
    for b in range(nb1):
        first = agg1[b] * reps
        piece = recvx[first]
        for t in range(1, reps):
            piece = piece + recvx[first + t]
        x1[b] = x1[b] + product(stacked(piece), phead1[b], ptail1[b], NT, loads)

    for _ in range(NU):
        pack(x1, send1, sends1, e1)
        start(*level1, e1)
        own_ext(x1, ext1, nb1)
        sweep1(e1, b1, x1)
        e1 += 1

    for b in range(nb1):
        ext1[b] = stacked(x1[b])
    for b in range(nb):
        x0[b] = x0[b] + product(ext1[agg0[b]], phead0[b], ptail0[b], NT, loads)
    for i in range(NU):
        pack(x0, send0, sends0, e0)
        start(*level0, e0)
        own_ext(x0, ext0, nb)
        sweep0(e0, out if i == NU - 1 else x0)
        e0 += 1

    for e in range(e0):
        drain(*level0, e)
    for e in range(e1):
        drain(*level1, e)
    all_bytes(recva, s_bsend.at[0])
    all_bytes(recvc, s_bsend.at[1])
    all_bytes(recvx, s_bsend.at[2])


def on_device(
    rhs, diag0, blocks0, cols0, sends0, pro0, agg0, diag1, blocks1, cols1, sends1, pro1, agg1, cinv
):
    n_row, n_col = lax.axis_size("row"), lax.axis_size("col")
    n = n_row * n_col
    _, _, nb, loads, bs = rhs.shape
    nb1 = diag1.shape[2]
    k0, k1 = cols0.shape[3], cols1.shape[3]
    g0, g1 = sends0.shape[3], sends1.shape[3]
    rounds = 2 * NU
    tall = -(-2 * loads // 16) * 16
    floats = [a[0, 0] for a in (rhs, diag0, blocks0, pro0, diag1, blocks1, pro1)] + [cinv]
    ints = [a[0, 0] for a in (cols0, sends0, agg0, cols1, sends1, agg1)]
    vm = pltpu.VMEM
    dma = pltpu.SemaphoreType.DMA
    scratch = [vm(a.shape, F32) for a in floats]
    scratch += [dma((nb + 7,))]
    scratch += [vm((nb, bs, k0 * bs), BF16)] * 2
    scratch += [vm((nb1, bs, k1 * bs), BF16)] * 2
    scratch += [vm((nb, bs, bs), BF16)] * 2
    scratch += [vm((nb1, bs, bs), BF16)] * 2
    scratch += [vm(cinv.shape, BF16)] * 2
    scratch += [vm((nb, loads, bs), F32)] * 2
    scratch += [vm((nb1, loads, bs), F32)] * 2
    scratch += [vm((nb + 4 * g0, tall, bs), BF16), vm((nb1 + 4 * g1, tall, bs), BF16)]
    scratch += [vm((nb, loads, bs), F32), vm((nb1, loads, bs), F32), vm((nb1, loads, bs), F32)]
    scratch += [vm((rounds, 4, g0, loads, bs), F32)] * 2
    scratch += [vm((rounds, 4, g1, loads, bs), F32)] * 2
    scratch += [vm((nb1 * loads, bs), F32), vm((n, nb1 * loads, bs), F32)] * 2
    scratch += [vm((loads, bs), F32), vm((n, loads, bs), F32)]
    scratch += [dma((rounds, 4))] * 4 + [dma((3,))] * 2
    result = pl.pallas_call(
        functools.partial(kernel, n_row, n_col),
        out_shape=jax.ShapeDtypeStruct((nb, loads, bs), F32),
        in_specs=[pl.BlockSpec(memory_space=pltpu.SMEM)] * 6
        + [pl.BlockSpec(memory_space=pl.ANY)] * 8,
        out_specs=pl.BlockSpec(memory_space=pltpu.VMEM),
        scratch_shapes=scratch,
        compiler_params=pltpu.CompilerParams(
            collective_id=0, has_side_effects=True, vmem_limit_bytes=60 * 1024 * 1024
        ),
    )(*ints, *floats)
    return result[None, None]


def solution(mesh):
    return jax.shard_map(
        on_device,
        mesh=mesh,
        in_specs=(
            P("row", "col", None, None, None),
            P("row", "col", None, None),
            P("row", "col", None, None, None, None),
            P("row", "col", None, None),
            P("row", "col", None, None),
            P("row", "col", None, None, None),
            P("row", "col", None),
            P("row", "col", None, None),
            P("row", "col", None, None, None, None),
            P("row", "col", None, None),
            P("row", "col", None, None),
            P("row", "col", None, None, None),
            P("row", "col", None),
            P(("row", "col"), None),
        ),
        out_specs=P("row", "col", None, None, None),
        check_vma=False,
    )
```

```python
import functools

import jax
import jax.numpy as jnp
from jax import lax
from jax.experimental import pallas as pl
from jax.experimental.pallas import tpu as pltpu
from jax.sharding import PartitionSpec as P

NU = 2
OMEGA = 0.3
F32 = jnp.float32
BF16 = jnp.bfloat16
MESH = pl.DeviceIdType.MESH
NT = (((1,), (1,)), ((), ()))
NN = (((1,), (0,)), ((), ()))


def two_terms(value):
    head = value.astype(BF16)
    tail = (value - head.astype(F32)).astype(BF16)
    return head, tail


def stacked(value):
    head = value.astype(BF16).astype(F32)
    rows = 2 * value.shape[0]
    pad = -rows % 16
    parts = [head, value - head]
    if pad:
        parts.append(jnp.zeros((pad, value.shape[1]), F32))
    return jnp.concatenate(parts, axis=0).astype(BF16)


def product(lhs, head, tail, dims, rows):
    both = lax.dot_general(lhs, head, dims, preferred_element_type=F32) + lax.dot_general(
        lhs, tail, dims, preferred_element_type=F32
    )
    return both[:rows] + both[rows : 2 * rows]


def kernel(
    n_row, n_col,
    cols0_h, sends0_h, agg0_h, cols1_h, sends1_h, agg1_h,
    rhs_h, diag0_h, blocks0_h, pro0_h, diag1_h, blocks1_h, pro1_h, cinv_h,
    out,
    rhs, diag0, blocks0, pro0, diag1, blocks1, pro1, cinv,
    cols0, sends0, agg0, cols1, sends1, agg1,
    in_sem,
    wide0, wide1, phead0, ptail0, phead1, ptail1, chead, ctail,
    dfull0, wfull0, dfull1, wfull1,
    ext0, ext1, x0, x1, b1,
    send0, recv0, send1, recv1,
    aggf, recva, mine, recvc, xs, recvx,
    s_send0, s_recv0, s_send1, s_recv1, s_bsend, s_brecv,
):
    nb, loads, bs = rhs.shape
    nb1 = diag1.shape[0]
    k0 = blocks0.shape[1]
    k1 = blocks1.shape[1]
    g0 = send0.shape[2]
    g1 = send1.shape[2]
    n = n_row * n_col
    owned = cinv.shape[0]
    ncb = cinv.shape[1] // bs
    reps = bs // owned
    row = lax.axis_index("row")
    col = lax.axis_index("col")
    me = row * n_col + col

    def peer(step):
        other = lax.rem(me + step, n)
        return (other // n_col, lax.rem(other, n_col))

    loading = []

    def load(source, target):
        copy = pltpu.make_async_copy(source, target, in_sem.at[len(loading)])
        loading.append(copy)
        copy.start()
        return copy

    l_ints = [
        load(source, target)
        for source, target in (
            (sends0_h, sends0), (cols0_h, cols0), (agg1_h, agg1),
            (agg0_h, agg0), (sends1_h, sends1), (cols1_h, cols1),
        )
    ]
    l_rhs = load(rhs_h, rhs)
    l_diag0 = load(diag0_h, diag0)
    l_blocks0 = [load(blocks0_h.at[b], blocks0.at[b]) for b in range(nb)]
    l_pro0 = load(pro0_h, pro0)
    l_diag1 = load(diag1_h, diag1)
    l_blocks1 = load(blocks1_h, blocks1)
    l_pro1 = load(pro1_h, pro1)
    l_cinv = load(cinv_h, cinv)

    recv0[...] = jnp.zeros_like(recv0)
    recv1[...] = jnp.zeros_like(recv1)

    barrier = pltpu.get_barrier_semaphore()

    def greet(step, carry):
        pl.semaphore_signal(barrier, inc=1, device_id=peer(step), device_id_type=MESH)
        return carry

    lax.fori_loop(1, n, greet, 0)

    directions = (
        (row < n_row - 1, (row + 1, col), row > 0),
        (row > 0, (row - 1, col), row < n_row - 1),
        (col < n_col - 1, (row, col + 1), col > 0),
        (col > 0, (row, col - 1), col < n_col - 1),
    )

    def halo_copy(send, recv, s_send, s_recv, e, d, there):
        return pltpu.make_async_remote_copy(
            src_ref=send.at[e, d], dst_ref=recv.at[e, d],
            send_sem=s_send.at[e, d], recv_sem=s_recv.at[e, d],
            device_id=there, device_id_type=MESH,
        )

    def pack(x, send, sends, e, flip=False):
        for d in range(4):
            for g in range(send.shape[2]):
                send[e, d, g] = x[sends[g, d] if flip else sends[d, g]]

    def start(send, recv, s_send, s_recv, e):
        for d, (goes, there, _) in enumerate(directions):
            @pl.when(goes)
            def _():
                halo_copy(send, recv, s_send, s_recv, e, d, there).start()

    def finish(send, recv, s_send, s_recv, e):
        for d, (_, there, comes) in enumerate(directions):
            @pl.when(comes)
            def _():
                halo_copy(send, recv, s_send, s_recv, e, d, (row, col)).wait_recv()

    def drain(send, recv, s_send, s_recv, e):
        for d, (goes, there, _) in enumerate(directions):
            @pl.when(goes)
            def _():
                halo_copy(send, recv, s_send, s_recv, e, d, there).wait_send()

    level0 = (send0, recv0, s_send0, s_recv0)
    level1 = (send1, recv1, s_send1, s_recv1)

    def own_ext(x, ext, count):
        for b in range(count):
            ext[b] = stacked(x[b])

    def ghost_ext(recv, ext, count, e):
        ghosts = recv.shape[2]
        for d in range(4):
            for g in range(ghosts):
                ext[count + d * ghosts + g] = stacked(recv[e, d, g])

    def coupled(b, cols, ext, wide, k):
        lhs = jnp.concatenate([ext[cols[b, i]] for i in range(k)], axis=1)
        both = lax.dot_general(lhs, wide[b], NN, preferred_element_type=F32)
        both = both[:, :bs] + both[:, bs:]
        return both[:loads] + both[loads : 2 * loads]

    def split_blocks(b, blocks, wide, k):
        def one(i, carry):
            h, t = two_terms(blocks[b, i].T)
            at = pl.ds(pl.multiple_of(i * bs, bs), bs)
            wide[b, at, :bs] = h
            wide[b, at, bs:] = t
            return carry

        lax.fori_loop(0, k, one, 0, unroll=7)

    l_rhs.wait()
    l_diag0.wait()
    for b in range(nb):
        d = jnp.broadcast_to(diag0[b : b + 1, :], (loads, bs))
        w = OMEGA / d
        dfull0[b] = d
        wfull0[b] = w
        x0[b] = w * rhs[b]
    for copy in l_ints:
        copy.wait()
    pack(x0, send0, sends0, 0)
    for b in range(nb1):
        aggf[b : b + 1, :] = jnp.full((1, bs), agg1[b].astype(F32))
    recva[me] = aggf[...]
    pl.semaphore_wait(barrier, n - 1)
    start(*level0, 0)

    def everywhere(src, dst, which):
        def one(there, carry):
            pltpu.make_async_remote_copy(
                src_ref=src, dst_ref=dst.at[me],
                send_sem=s_bsend.at[which], recv_sem=s_brecv.at[which],
                device_id=there, device_id_type=MESH,
            ).start()
            return carry

        half = n_col // 2
        side = col // half

        def far(i, carry):
            across = (1 - side) * half + lax.rem(col + i // n_row, half)
            return one((lax.rem(row + i, n_row), across), carry)

        def near(i, carry):
            beside = side * half + lax.rem(col + i // n_row, half)
            return one((lax.rem(row + i, n_row), beside), carry)

        lax.fori_loop(0, n_row * half, far, 0)
        lax.fori_loop(1, n_row * half, near, 0)

    def all_bytes(dst, sem):
        part = dst.at[pl.ds(0, n - 1)]
        pltpu.make_async_copy(part, part, sem).wait()

    everywhere(aggf, recva, 0)
    own_ext(x0, ext0, nb)
    def arrive(b):
        l_blocks0[b].wait()
        split_blocks(b, blocks0, wide0, k0)

    early = nb
    for b in range(early):
        arrive(b)

    def sweep0(e, into):
        finish(*level0, e)
        ghost_ext(recv0, ext0, nb, e)
        for b in range(nb):
            if e == 0 and b + early < nb:
                arrive(b + early)
            c = coupled(b, cols0, ext0, wide0, k0)
            v = x0[b]
            into[b] = v + wfull0[b] * (rhs[b] - (dfull0[b] * v + c))

    def sweep1(e, right, into):
        finish(*level1, e)
        ghost_ext(recv1, ext1, nb1, e)
        for b in range(nb1):
            c = coupled(b, cols1, ext1, wide1, k1)
            v = x1[b]
            into[b] = v + wfull1[b] * (right[b] - (dfull1[b] * v + c))

    e0 = 0
    for _ in range(NU - 1):
        sweep0(e0, x0)
        e0 += 1
        pack(x0, send0, sends0, e0)
        start(*level0, e0)
        own_ext(x0, ext0, nb)

    l_pro0.wait()
    for b in range(nb):
        h, t = two_terms(pro0[b])
        phead0[b] = h
        ptail0[b] = t
    l_blocks1.wait()
    for b in range(nb1):
        split_blocks(b, blocks1, wide1, k1)
    l_diag1.wait()
    for b in range(nb1):
        d = jnp.broadcast_to(diag1[b : b + 1, :], (loads, bs))
        dfull1[b] = d
        wfull1[b] = OMEGA / d

    finish(*level0, e0)
    ghost_ext(recv0, ext0, nb, e0)
    sums = [jnp.zeros((loads, bs), F32) for _ in range(nb1)]
    for b in range(nb):
        c = coupled(b, cols0, ext0, wide0, k0)
        r = rhs[b] - (dfull0[b] * x0[b] + c)
        q = product(stacked(r), phead0[b], ptail0[b], NN, loads)
        for a in range(nb1):
            sums[a] = sums[a] + jnp.where(agg0[b] == a, q, 0.0)
    e0 += 1

    for b in range(nb1):
        b1[b] = sums[b]
        x1[b] = wfull1[b] * sums[b]
    pack(x1, send1, sends1, 0, True)
    start(*level1, 0)
    own_ext(x1, ext1, nb1)
    l_pro1.wait()
    for b in range(nb1):
        h, t = two_terms(pro1[b])
        phead1[b] = h
        ptail1[b] = t
    l_cinv.wait()
    h, t = two_terms(cinv[...])
    chead[...] = h
    ctail[...] = t
    e1 = 0
    for _ in range(NU - 1):
        sweep1(e1, b1, x1)
        e1 += 1
        pack(x1, send1, sends1, e1, True)
        start(*level1, e1)
        own_ext(x1, ext1, nb1)
    finish(*level1, e1)
    ghost_ext(recv1, ext1, nb1, e1)
    for b in range(nb1):
        c = coupled(b, cols1, ext1, wide1, k1)
        r = b1[b] - (dfull1[b] * x1[b] + c)
        q = product(stacked(r), phead1[b], ptail1[b], NN, loads)
        mine[b * loads : (b + 1) * loads, :] = q
    e1 += 1

    everywhere(mine, recvc, 1)
    recvc[me] = mine[...]
    all_bytes(recva, s_brecv.at[0])
    all_bytes(recvc, s_brecv.at[1])
    index = lax.broadcasted_iota(jnp.int32, (ncb, nb1 * loads, bs), 0).astype(F32)

    def collect(d, total):
        names = recva[d]
        names = jnp.concatenate(
            [jnp.broadcast_to(names[b : b + 1], (loads, bs)) for b in range(nb1)], axis=0
        )
        return total + jnp.where(names[None] == index, recvc[d][None], 0.0)

    total = lax.fori_loop(
        0, n, collect, jnp.zeros((ncb, nb1 * loads, bs), F32), unroll=4
    )
    pieces = []
    for c in range(ncb):
        piece = total[c, :loads]
        for b in range(1, nb1):
            piece = piece + total[c, b * loads : (b + 1) * loads]
        pieces.append(stacked(piece))
    own = product(jnp.concatenate(pieces, axis=1), chead[...], ctail[...], NT, loads)
    wide = jnp.concatenate([own] * reps, axis=1)
    group = lax.broadcasted_iota(jnp.int32, (loads, bs), 1) // owned
    diagonal = group == lax.broadcasted_iota(jnp.int32, (loads, bs), 0)
    xs[...] = jnp.sum(jnp.where(diagonal, wide, 0.0), axis=0, keepdims=True)
    everywhere(xs, recvx, 2)
    recvx[me] = xs[...]
    all_bytes(recvx, s_brecv.at[2])
    for b in range(nb1):
        first = agg1[b] * reps
        parts = jnp.concatenate([recvx[first + t] for t in range(reps)], axis=0)
        piece = jnp.where(diagonal, parts, 0.0)
        for t in range(1, reps):
            turned = jnp.concatenate(
                [parts[:, bs - t * owned :], parts[:, : bs - t * owned]], axis=1
            )
            turned = jnp.where(diagonal, turned, 0.0)
            piece = piece + jnp.concatenate([turned[t:], turned[:t]], axis=0)
        x1[b] = x1[b] + product(stacked(piece), phead1[b], ptail1[b], NT, loads)

    for _ in range(NU):
        pack(x1, send1, sends1, e1, True)
        start(*level1, e1)
        own_ext(x1, ext1, nb1)
        sweep1(e1, b1, x1)
        e1 += 1

    for b in range(nb1):
        ext1[b] = stacked(x1[b])
    for b in range(nb):
        x0[b] = x0[b] + product(ext1[agg0[b]], phead0[b], ptail0[b], NT, loads)
    for i in range(NU):
        pack(x0, send0, sends0, e0)
        start(*level0, e0)
        own_ext(x0, ext0, nb)
        sweep0(e0, out if i == NU - 1 else x0)
        e0 += 1

    for e in range(e0):
        drain(*level0, e)
    for e in range(e1):
        drain(*level1, e)
    all_bytes(recva, s_bsend.at[0])
    all_bytes(recvc, s_bsend.at[1])
    all_bytes(recvx, s_bsend.at[2])


def on_device(
    rhs, diag0, blocks0, cols0, sends0, pro0, agg0, diag1, blocks1, cols1, sends1, pro1, agg1, cinv
):
    n_row, n_col = lax.axis_size("row"), lax.axis_size("col")
    n = n_row * n_col
    _, _, nb, loads, bs = rhs.shape
    nb1 = diag1.shape[2]
    k0, k1 = cols0.shape[3], cols1.shape[3]
    g0, g1 = sends0.shape[3], sends1.shape[3]
    rounds = 2 * NU
    tall = -(-2 * loads // 16) * 16
    floats = [a[0, 0] for a in (rhs, diag0, blocks0, pro0, diag1, blocks1, pro1)] + [cinv]
    ints = [a[0, 0] for a in (cols0, sends0, agg0, cols1)]
    ints += [sends1[0, 0].T, agg1[0, 0]]
    vm = pltpu.VMEM
    dma = pltpu.SemaphoreType.DMA
    scratch = [vm(a.shape, F32) for a in floats]
    scratch += [pltpu.SMEM(a.shape, jnp.int32) for a in ints]
    scratch += [dma((nb + 7 + len(ints),))]
    scratch += [vm((nb, k0 * bs, 2 * bs), BF16), vm((nb1, k1 * bs, 2 * bs), BF16)]
    scratch += [vm((nb, bs, bs), BF16)] * 2
    scratch += [vm((nb1, bs, bs), BF16)] * 2
    scratch += [vm(cinv.shape, BF16)] * 2
    scratch += [vm((nb, loads, bs), F32)] * 2
    scratch += [vm((nb1, loads, bs), F32)] * 2
    scratch += [vm((nb + 4 * g0, tall, bs), BF16), vm((nb1 + 4 * g1, tall, bs), BF16)]
    scratch += [vm((nb, loads, bs), F32), vm((nb1, loads, bs), F32), vm((nb1, loads, bs), F32)]
    scratch += [vm((rounds, 4, g0, loads, bs), F32)] * 2
    scratch += [vm((rounds, 4, g1, loads, bs), F32)] * 2
    scratch += [vm((nb1, bs), F32), vm((n, nb1, bs), F32)]
    scratch += [vm((nb1 * loads, bs), F32), vm((n, nb1 * loads, bs), F32)]
    scratch += [vm((1, bs), F32), vm((n, 1, bs), F32)]
    scratch += [dma((rounds, 4))] * 4 + [dma((3,))] * 2
    result = pl.pallas_call(
        functools.partial(kernel, n_row, n_col),
        out_shape=jax.ShapeDtypeStruct((nb, loads, bs), F32),
        in_specs=[pl.BlockSpec(memory_space=pl.ANY)] * 14,
        out_specs=pl.BlockSpec(memory_space=pltpu.VMEM),
        scratch_shapes=scratch,
        compiler_params=pltpu.CompilerParams(
            collective_id=0, has_side_effects=True, vmem_limit_bytes=60 * 1024 * 1024
        ),
    )(*ints, *floats)
    return result[None, None]


def solution(mesh):
    return jax.shard_map(
        on_device,
        mesh=mesh,
        in_specs=(
            P("row", "col", None, None, None),
            P("row", "col", None, None),
            P("row", "col", None, None, None, None),
            P("row", "col", None, None),
            P("row", "col", None, None),
            P("row", "col", None, None, None),
            P("row", "col", None),
            P("row", "col", None, None),
            P("row", "col", None, None, None, None),
            P("row", "col", None, None),
            P("row", "col", None, None),
            P("row", "col", None, None, None),
            P("row", "col", None),
            P(("row", "col"), None),
        ),
        out_specs=P("row", "col", None, None, None),
        check_vma=False,
    )
```
